32 devices in a mesh: rows: 4 (over y, x), mp: 8 (over z, core).
Axes of the slice: x: 2, y: 2, z: 4, core: 2. Of those that a mesh axis runs over, the one named last changes fastest.
Arguments:
- tokens: bfloat16 [512, 6144], P('rows', 'mp'), may hold values from -8 to 8
- norm_gain: float32 [6144], replicated, may hold values from 0.25 to 1.75
- hidden_bias: float32 [24576], P('mp'), may hold values from -3 to 3
- weight_in: bfloat16 [6144, 24576], P('rows', 'mp'), may hold values from -0.078125 to 0.078125
- weight_out: bfloat16 [24576, 6144], P('mp', 'rows'), may hold values from -0.0546875 to 0.0546875
Outputs:
- updated: bfloat16 [512, 6144], P('rows', 'mp')
The draws below stay inside these ranges and needn't reach their ends.
All inputs are finite; a program needn't handle non-finite values.
Results may differ from the reference program's by a relative error of at most 0.0041.
Values may be sent and summed in bfloat16 or wider, within the bound.
No kernel may reach another device: no remote copies, remote signals or barrier semaphores. Data moves between devices by JAX's collectives and lax.ppermute only.
A program may use at most 128 MiB of HBM per device.

```python
import jax
import jax.numpy as jnp
from jax import lax

D = 6144
FF = 24576
TOKENS = 512


def raised(array, own_key, source, target, blocks, factor):
    owner, partner = [(jnp.arange(array.shape[position]) // (array.shape[position] // blocks)).reshape([-1 if axis == position else 1 for axis in range(array.ndim)]) for position in (source, target)]
    chosen = jax.random.permutation(own_key, blocks)[partner]
    strong = (owner == chosen) | (owner == (partner + blocks // 2) % blocks)
    return jnp.where(strong, factor * array, array)


def block_scale(own_key, extent, cuts, smallest, high):
    factor_of = 1.0
    for dim, blocks in cuts:
        heights = jax.random.uniform(jax.random.fold_in(jax.random.fold_in(own_key, 6), dim), (blocks,), jnp.float32, smallest / len(cuts), high / len(cuts))
        factor_of = factor_of * jnp.repeat(jnp.exp(heights), extent[dim] // blocks).reshape((-1,) + (1,) * (len(extent) - 1 - dim))
    return factor_of


def gaussian(own_key, extent, spread, limit, split=(), dtype=jnp.bfloat16):
    array = spread * jax.random.normal(own_key, extent, jnp.float32)
    if split:
        array = array * block_scale(own_key, extent, split, -0.22, 0.18)
    return jnp.clip(array, -limit, limit).astype(dtype)


def heavy_noise(stream_key, extent, spread, reach, shards, heavy, kind=jnp.bfloat16):
    array = spread * jax.random.normal(stream_key, extent, jnp.float32)
    if shards:
        array = array * block_scale(stream_key, extent, shards, -0.22, 0.18)
    return jnp.clip(raised(array, jax.random.fold_in(stream_key, 3), *heavy), -reach, reach).astype(kind)


def setup_inputs(seed: int = 0) -> dict:
    streams_of = jax.random.split(jax.random.key(seed), 6)
    return {
        "tokens": heavy_noise(streams_of[0], (TOKENS, D), 1.0, 8.0, ((0, 4), (1, 8)), (1, 0, 8, 2.0)),
        "norm_gain": jnp.clip(1.0 + 0.15 * jax.random.normal(streams_of[1], (D,), jnp.float32), 0.25, 1.75),
        "hidden_bias": gaussian(streams_of[2], (FF,), 0.5, 3.0, ((0, 8),), jnp.float32),
        "weight_in": gaussian(streams_of[3], (D, FF), D ** -0.5, 0.078125, ((0, 4), (1, 8))),
        "weight_out": heavy_noise(streams_of[4], (FF, D), FF ** -0.5, 0.0546875, ((0, 8), (1, 4)), (0, 1, 8, 2.0)),
    }


floor_value = 0.1

def normalize(as_float, moment_sum, square_sum, gain, width):
    row_mean = moment_sum / width
    row_var = jnp.maximum(square_sum / width - row_mean * row_mean, 0.0)
    inverse = lax.rsqrt(row_var + floor_value)
    return ((as_float - row_mean[:, None]) * inverse[:, None] * gain[None, :]).astype(jnp.bfloat16)

def reference(tokens, norm_gain, hidden_bias, weight_in, weight_out):
    as_float = tokens.astype(jnp.float32)
    normed = normalize(as_float, lax.optimization_barrier(jnp.sum(as_float, axis=1)), lax.optimization_barrier(jnp.sum(as_float * as_float, axis=1)), norm_gain, D)
    preact = jnp.dot(normed, weight_in, preferred_element_type=jnp.float32) + hidden_bias[None, :]
    hidden = jax.nn.gelu(preact, approximate=False).astype(jnp.bfloat16)
    branch = jnp.dot(hidden, weight_out, preferred_element_type=jnp.float32)
    return (as_float + branch).astype(jnp.bfloat16)
```

```python
import jax
import jax.numpy as jnp
from jax import lax
from jax.sharding import PartitionSpec as P


floor_value = 0.1
CORES = 2
TOKEN_CHUNKS = 1
COLUMN_CHUNKS = 4


def make_body(rows, mp):
    depth = mp // CORES
    bits = [1 << n for n in range(rows.bit_length() - 1)]

    def over_rows(value, flip):
        return lax.ppermute(value, "rows", [(i, i ^ flip) for i in range(rows)])

    def over_cores(value):
        return lax.ppermute(value, "mp", [(i, i ^ 1) for i in range(mp)])

    def over_depth(value, shift):
        return lax.ppermute(value, "mp", [(i, (i + CORES * shift) % mp) for i in range(mp)])

    def gather_depth(block):
        got = {0: block}
        up = down = block
        half = block.shape[0] // 2
        for step in range(1, depth // 2):
            up, down = over_depth(up, 1), over_depth(down, -1)
            got[step], got[depth - step] = up, down
        if depth > 1:
            top, bottom = over_depth(up[:half], 1), over_depth(down[half:], -1)
            got[depth // 2] = jnp.concatenate([top, bottom], axis=0)
        return [got[j] for j in range(depth)]

    def scatter_depth(parts):
        half = parts[0].shape[0] // 2
        middle = parts[depth // 2]
        up = down = None
        for distance in range(depth // 2, 0, -1):
            if distance == depth // 2:
                give_up, give_down = middle[:half], middle[half:]
            else:
                mine_up, mine_down = parts[depth - distance], parts[distance]
                if distance == depth // 2 - 1:
                    give_up = jnp.concatenate([mine_up[:half] + up, mine_up[half:]], axis=0)
                    give_down = jnp.concatenate([mine_down[:half], mine_down[half:] + down], axis=0)
                else:
                    give_up, give_down = mine_up + up, mine_down + down
            up = over_depth(give_up.astype(jnp.bfloat16), 1).astype(jnp.float32)
            down = over_depth(give_down.astype(jnp.bfloat16), -1).astype(jnp.float32)
        return parts[0] + up + down

    def body(tokens, norm_gain, hidden_bias, weight_in, weight_out):
        count, width = tokens.shape
        hidden_width = weight_in.shape[1]
        per_row = depth // rows
        features = width * mp
        row, place = lax.axis_index("rows"), lax.axis_index("mp")
        core, chip = place % CORES, place // CORES

        as_float = tokens.astype(jnp.float32)
        sums = jnp.stack([jnp.sum(as_float, axis=1), jnp.sum(as_float * as_float, axis=1)])
        sums = sums + over_cores(sums)
        sums = sum([over_depth(sums, shift) for shift in range(1, depth)], sums)
        row_mean = sums[0] / features
        row_var = jnp.maximum(sums[1] / features - row_mean * row_mean, 0.0)
        inverse = lax.rsqrt(row_var + floor_value)

        gains = lax.dynamic_index_in_dim(norm_gain.reshape(depth, CORES, width), core, 1, keepdims=False)
        win = weight_in.reshape(per_row, CORES, width, hidden_width)
        wout = weight_out.reshape(hidden_width, per_row, CORES, width)
        win_own = lax.dynamic_index_in_dim(win, core, 1, keepdims=False).reshape(per_row * width, hidden_width)
        win_other = lax.dynamic_index_in_dim(win, 1 - core, 1, keepdims=False).reshape(per_row * width, hidden_width)
        wout_own = lax.dynamic_index_in_dim(wout, core, 2, keepdims=False).reshape(hidden_width, per_row * width)
        wout_other = lax.dynamic_index_in_dim(wout, 1 - core, 2, keepdims=False).reshape(hidden_width, per_row * width)

        rows_here = count // TOKEN_CHUNKS
        cols_here = hidden_width // COLUMN_CHUNKS
        results = []
        for t in range(TOKEN_CHUNKS):
            span = slice(t * rows_here, (t + 1) * rows_here)
            stacked = jnp.stack(gather_depth(tokens[span]))
            mean_t, inverse_t = row_mean[span], inverse[span]
            pieces = []
            for flip in range(rows):
                to = row ^ flip
                parts = []
                for sub in range(per_row):
                    at = to * per_row + sub
                    raw = lax.dynamic_index_in_dim(stacked, (chip - at) % depth, 0, keepdims=False).astype(jnp.float32)
                    gain = lax.dynamic_index_in_dim(gains, at, 0, keepdims=False)
                    parts.append(((raw - mean_t[:, None]) * inverse_t[:, None] * gain[None, :]).astype(jnp.bfloat16))
                piece = parts[0] if per_row == 1 else jnp.concatenate(parts, axis=1)
                pieces.append(over_rows(piece, flip) if flip else piece)
            x_own = jnp.concatenate(pieces, axis=0)
            x_other = over_cores(x_own)

            own = other = 0.0
            for c in range(COLUMN_CHUNKS):
                cols = slice(c * cols_here, (c + 1) * cols_here)
                order = bits[c % len(bits):] + bits[: c % len(bits)]
                part = jnp.dot(x_own, win_own[:, cols], preferred_element_type=jnp.float32) + jnp.dot(
                    x_other, win_other[:, cols], preferred_element_type=jnp.float32
                )
                held = {b: part[b * rows_here : (b + 1) * rows_here] for b in range(rows)}
                for bit in order:
                    going = [b for b in held if b & bit]
                    sent = over_rows(jnp.concatenate([held[b].astype(jnp.bfloat16) for b in going], axis=0), bit)
                    held = {
                        b ^ bit: held[b ^ bit] + sent[n * rows_here : (n + 1) * rows_here].astype(jnp.float32)
                        for n, b in enumerate(going)
                    }
                hidden = jax.nn.gelu(held[0] + hidden_bias[None, cols], approximate=False).astype(jnp.bfloat16)
                names, block = [0], hidden
                for bit in reversed(order):
                    names = names + [b ^ bit for b in names]
                    block = jnp.concatenate([block, over_rows(block, bit)], axis=0)
                places = {b: n for n, b in enumerate(names)}
                if names != sorted(names):
                    block = jnp.concatenate([block[places[b] * rows_here : (places[b] + 1) * rows_here] for b in range(rows)], axis=0)
                other = other + jnp.dot(block, wout_other[cols], preferred_element_type=jnp.float32)
                own = own + jnp.dot(block, wout_own[cols], preferred_element_type=jnp.float32)

            total = own + over_cores(other.astype(jnp.bfloat16)).astype(jnp.float32)
            backs = []
            for flip in range(rows):
                piece = total[flip * rows_here : (flip + 1) * rows_here].astype(jnp.bfloat16)
                backs.append(over_rows(piece, flip) if flip else piece)
            blocks = jnp.stack(backs).reshape(rows, rows_here, per_row, width)
            blocks = jnp.moveaxis(blocks, 2, 1).reshape(depth, rows_here, width)
            parts = []
            for j in range(depth):
                target = (chip - j) % depth
                index = ((target // per_row) ^ row) * per_row + target % per_row
                parts.append(lax.dynamic_index_in_dim(blocks, index, 0, keepdims=False).astype(jnp.float32))
            results.append((as_float[span] + scatter_depth(parts)).astype(jnp.bfloat16))
        return results[0] if TOKEN_CHUNKS == 1 else jnp.concatenate(results, axis=0)

    return body


def solution(mesh):
    return jax.shard_map(
        make_body(mesh.shape["rows"], mesh.shape["mp"]),
        mesh=mesh,
        in_specs=(P("rows", "mp"), P(), P("mp"), P("rows", "mp"), P("mp", "rows")),
        out_specs=P("rows", "mp"),
        check_vma=False,
    )
```

```python
import jax
import jax.numpy as jnp
from jax import lax
from jax.sharding import PartitionSpec as P


floor_value = 0.1
CORES = 2
TOKEN_CHUNKS = 2
COLUMN_CHUNKS = 2


def make_body(rows, mp):
    depth = mp // CORES
    per_row = depth // rows
    bits = [1 << n for n in range(rows.bit_length() - 1)]

    def over_rows(value, flip):
        return lax.ppermute(value, "rows", [(i, i ^ flip) for i in range(rows)])

    def over_cores(value):
        return lax.ppermute(value, "mp", [(i, i ^ 1) for i in range(mp)])

    def over_depth(value, shift):
        return lax.ppermute(value, "mp", [(i, (i + CORES * shift) % mp) for i in range(mp)])

    def spread(value, j):
        pairs = []
        for r in range(rows):
            for m in range(mp):
                z, core = divmod(m, CORES)
                target = (r * per_row + z % per_row) ^ j
                pairs.append((r * mp + m, (z // per_row) * mp + target * CORES + core))
        return lax.ppermute(value, ("rows", "mp"), pairs)

    def scatter_depth(parts):
        half = parts[0].shape[0] // 2
        middle = parts[depth // 2]
        up = down = None
        for distance in range(depth // 2, 0, -1):
            if distance == depth // 2:
                give_up, give_down = middle[:half], middle[half:]
            else:
                mine_up, mine_down = parts[depth - distance], parts[distance]
                if distance == depth // 2 - 1:
                    give_up = jnp.concatenate([mine_up[:half] + up, mine_up[half:]], axis=0)
                    give_down = jnp.concatenate([mine_down[:half], mine_down[half:] + down], axis=0)
                else:
                    give_up, give_down = mine_up + up, mine_down + down
            up = over_depth(give_up.astype(jnp.bfloat16), 1).astype(jnp.float32)
            down = over_depth(give_down.astype(jnp.bfloat16), -1).astype(jnp.float32)
        return parts[0] + up + down

    def body(tokens, norm_gain, hidden_bias, weight_in, weight_out):
        count, width = tokens.shape
        hidden_width = weight_in.shape[1]
        features = width * mp
        row, place = lax.axis_index("rows"), lax.axis_index("mp")
        core, chip = place % CORES, place // CORES

        as_float = tokens.astype(jnp.float32)
        sums = jnp.stack([jnp.sum(as_float, axis=1), jnp.sum(as_float * as_float, axis=1)])
        sums = sums + over_cores(sums)
        sums = jnp.stack([over_rows(sums, flip) if flip else sums for flip in range(rows)])
        sums = sum([over_depth(sums, shift) for shift in range(1, depth)], sums)
        row_mean = sums[:, 0] / features
        row_var = jnp.maximum(sums[:, 1] / features - row_mean * row_mean, 0.0)
        inverse = lax.rsqrt(row_var + floor_value)

        gains = lax.dynamic_slice_in_dim(norm_gain, row * (features // rows), features // rows).reshape(per_row, CORES, width)
        gains = lax.dynamic_index_in_dim(gains, core, 1, keepdims=False)

        got = []
        for j in range(depth):
            got.append(spread(tokens, j))
        stacked = jnp.stack(got)
        pieces = []
        for flip in range(rows):
            parts = []
            for sub in range(per_row):
                at = ((row ^ flip) * per_row + sub) ^ chip
                raw = lax.dynamic_index_in_dim(stacked, at, 0, keepdims=False).astype(jnp.float32)
                scaled = (raw - row_mean[flip][:, None]) * inverse[flip][:, None] * gains[sub][None, :]
                parts.append(scaled.astype(jnp.bfloat16))
            pieces.append(parts)
        x_own = [jnp.concatenate([p[sub] for p in pieces], axis=0) for sub in range(per_row)]
        x_own = x_own[0] if per_row == 1 else jnp.concatenate(x_own, axis=1)
        x_other = over_cores(x_own)
        first = core == 0
        columns = []
        for sub in range(per_row):
            at = slice(sub * width, (sub + 1) * width)
            columns.append(jnp.where(first, x_own[:, at], x_other[:, at]))
            columns.append(jnp.where(first, x_other[:, at], x_own[:, at]))
        x_all = jnp.concatenate(columns, axis=1).reshape(rows, count, features // rows)

        rows_here = count // TOKEN_CHUNKS
        cols_here = hidden_width // COLUMN_CHUNKS
        results = []
        for t in range(TOKEN_CHUNKS):
            span = slice(t * rows_here, (t + 1) * rows_here)
            x_here = x_all[:, span].reshape(rows * rows_here, features // rows)
            terms = 0.0
            for c in range(COLUMN_CHUNKS):
                cols = slice(c * cols_here, (c + 1) * cols_here)
                order = bits[c % len(bits):] + bits[: c % len(bits)]
                part = jnp.dot(x_here, weight_in[:, cols], preferred_element_type=jnp.float32)
                held = {b: part[b * rows_here : (b + 1) * rows_here] for b in range(rows)}
                for bit in order:
                    going = [b for b in held if b & bit]
                    sent = over_rows(jnp.concatenate([held[b].astype(jnp.bfloat16) for b in going], axis=0), bit)
                    held = {
                        b ^ bit: held[b ^ bit] + sent[n * rows_here : (n + 1) * rows_here].astype(jnp.float32)
                        for n, b in enumerate(going)
                    }
                hidden = jax.nn.gelu(held[0] + hidden_bias[None, cols], approximate=False).astype(jnp.bfloat16)
                names, block = [0], hidden
                for bit in reversed(order):
                    names = names + [b ^ bit for b in names]
                    block = jnp.concatenate([block, over_rows(block, bit)], axis=0)
                places = {b: n for n, b in enumerate(names)}
                if names != sorted(names):
                    block = jnp.concatenate([block[places[b] * rows_here : (places[b] + 1) * rows_here] for b in range(rows)], axis=0)
                terms = terms + jnp.dot(block, weight_out[cols], preferred_element_type=jnp.float32)

            terms = [terms[:, n * width : (n + 1) * width] for n in range(per_row * CORES)]
            lower = terms[0::CORES][0] if per_row == 1 else jnp.concatenate(terms[0::CORES], axis=1)
            upper = terms[1::CORES][0] if per_row == 1 else jnp.concatenate(terms[1::CORES], axis=1)
            given = jnp.where(first, upper, lower).astype(jnp.bfloat16)
            total = jnp.where(first, lower, upper) + over_cores(given).astype(jnp.float32)
            backs = []
            for flip in range(rows):
                piece = total[flip * rows_here : (flip + 1) * rows_here].astype(jnp.bfloat16)
                backs.append(over_rows(piece, flip) if flip else piece)
            blocks = jnp.stack(backs).reshape(rows, rows_here, per_row, width)
            blocks = jnp.moveaxis(blocks, 2, 1).reshape(depth, rows_here, width)
            parts = []
            for j in range(depth):
                target = (chip - j) % depth
                index = ((target // per_row) ^ row) * per_row + target % per_row
                parts.append(lax.dynamic_index_in_dim(blocks, index, 0, keepdims=False).astype(jnp.float32))
            results.append((as_float[span] + scatter_depth(parts)).astype(jnp.bfloat16))
        return results[0] if TOKEN_CHUNKS == 1 else jnp.concatenate(results, axis=0)

    return body


def solution(mesh):
    rows, mp = mesh.shape["rows"], mesh.shape["mp"]
    inner = make_body(rows, mp)

    return jax.shard_map(
        inner,
        mesh=mesh,
        in_specs=(P("rows", "mp"), P(), P("mp"), P("rows", "mp"), P("mp", "rows")),
        out_specs=P("rows", "mp"),
        check_vma=False,
    )
```

```python
import jax
import jax.numpy as jnp
from jax import lax
from jax.sharding import PartitionSpec as P


floor_value = 0.1
CORES = 2
TOKEN_CHUNKS = 2
COLUMN_CHUNKS = 3
HALVES = True


def joined(parts, axis):
    return parts[0] if len(parts) == 1 else jnp.concatenate(parts, axis=axis)


def make_body(rows, mp):
    depth = mp // CORES
    per_row = depth // rows
    bits = [1 << n for n in range(rows.bit_length() - 1)]

    def over_rows(value, flip):
        return lax.ppermute(value, "rows", [(i, i ^ flip) for i in range(rows)])

    def over_cores(value):
        return lax.ppermute(value, "mp", [(i, i ^ 1) for i in range(mp)])

    def over_depth(value, shift):
        return lax.ppermute(value, "mp", [(i, (i + CORES * shift) % mp) for i in range(mp)])

    def spread(value, j):
        pairs = []
        for r in range(rows):
            for m in range(mp):
                z, core = divmod(m, CORES)
                target = (r * per_row + z % per_row) ^ j
                pairs.append((r * mp + m, (z // per_row) * mp + target * CORES + core))
        return lax.ppermute(value, ("rows", "mp"), pairs)

    def scatter_depth(parts):
        half = parts[0].shape[0] // 2
        middle = parts[depth // 2]
        up = down = None
        for distance in range(depth // 2, 0, -1):
            if distance == depth // 2:
                give_up, give_down = middle[:half], middle[half:]
            else:
                mine_up, mine_down = parts[depth - distance], parts[distance]
                if distance == depth // 2 - 1:
                    give_up = jnp.concatenate([mine_up[:half] + up, mine_up[half:]], axis=0)
                    give_down = jnp.concatenate([mine_down[:half], mine_down[half:] + down], axis=0)
                else:
                    give_up, give_down = mine_up + up, mine_down + down
            up = over_depth(give_up.astype(jnp.bfloat16), 1).astype(jnp.float32)
            down = over_depth(give_down.astype(jnp.bfloat16), -1).astype(jnp.float32)
        return parts[0] + up + down

    def body(tokens, norm_gain, hidden_bias, weight_in, weight_out):
        count, width = tokens.shape
        hidden_width = weight_in.shape[1]
        features = width * mp
        row, place = lax.axis_index("rows"), lax.axis_index("mp")
        core, chip = place % CORES, place // CORES
        first = core == 0

        as_float = tokens.astype(jnp.float32)
        sums = jnp.stack([jnp.sum(as_float, axis=1), jnp.sum(as_float * as_float, axis=1)])
        sums = lax.all_to_all(jnp.broadcast_to(sums, (rows * mp,) + sums.shape), ("rows", "mp"), 0, 0)
        sums = jnp.sum(sums.reshape((rows, mp) + sums.shape[1:]), axis=1)
        sums = jnp.stack([lax.dynamic_index_in_dim(sums, row ^ flip, 0, keepdims=False) for flip in range(rows)])
        row_mean = sums[:, 0] / features
        row_var = jnp.maximum(sums[:, 1] / features - row_mean * row_mean, 0.0)
        inverse = lax.rsqrt(row_var + floor_value)

        gains = lax.dynamic_slice_in_dim(norm_gain, row * (features // rows), features // rows).reshape(per_row, CORES, width)
        gains = lax.dynamic_index_in_dim(gains, core, 1, keepdims=False)

        got = []
        for j in range(depth):
            got.append(spread(tokens, j))
        stacked = jnp.stack(got)
        pieces = []
        for flip in range(rows):
            parts = []
            for sub in range(per_row):
                at = ((row ^ flip) * per_row + sub) ^ chip
                raw = lax.dynamic_index_in_dim(stacked, at, 0, keepdims=False).astype(jnp.float32)
                scaled = (raw - row_mean[flip][:, None]) * inverse[flip][:, None] * gains[sub][None, :]
                parts.append(scaled.astype(jnp.bfloat16))
            pieces.append(parts)
        x_own = joined([jnp.concatenate([p[sub] for p in pieces], axis=0) for sub in range(per_row)], 1)
        x_other = over_cores(x_own)

        if HALVES:
            blocks_in = weight_in.reshape(per_row, CORES, width, hidden_width)
            w_own = lax.dynamic_index_in_dim(blocks_in, core, 1, keepdims=False).reshape(per_row * width, hidden_width)
            w_other = lax.dynamic_index_in_dim(blocks_in, 1 - core, 1, keepdims=False).reshape(per_row * width, hidden_width)
            w_own, w_other = lax.optimization_barrier((w_own, w_other))
            x_all = [x.reshape(rows, count, per_row * width) for x in (x_own, x_other)]
            w_all = [w_own, w_other]
        else:
            columns = []
            for sub in range(per_row):
                at = slice(sub * width, (sub + 1) * width)
                columns.append(jnp.where(first, x_own[:, at], x_other[:, at]))
                columns.append(jnp.where(first, x_other[:, at], x_own[:, at]))
            x_all = [jnp.concatenate(columns, axis=1).reshape(rows, count, features // rows)]
            w_all = [weight_in]

        rows_here = count // TOKEN_CHUNKS
        cols_here = hidden_width // COLUMN_CHUNKS
        results = []
        for t in range(TOKEN_CHUNKS):
            span = slice(t * rows_here, (t + 1) * rows_here)
            terms = 0.0
            for c in range(COLUMN_CHUNKS):
                cols = slice(c * cols_here, (c + 1) * cols_here)
                turn = (c + t) % len(bits)
                order = bits[turn:] + bits[:turn]
                part = 0.0
                for x, w in zip(x_all, w_all):
                    x = x[:, span].reshape(rows * rows_here, x.shape[2])
                    part = part + jnp.dot(x, w[:, cols], preferred_element_type=jnp.float32)
                held = {b: part[b * rows_here : (b + 1) * rows_here] for b in range(rows)}
                for bit in order:
                    going = [b for b in held if b & bit]
                    sent = over_rows(jnp.concatenate([held[b].astype(jnp.bfloat16) for b in going], axis=0), bit)
                    held = {
                        b ^ bit: held[b ^ bit] + sent[k * rows_here : (k + 1) * rows_here].astype(jnp.float32)
                        for k, b in enumerate(going)
                    }
                hidden = jax.nn.gelu(held[0] + hidden_bias[None, cols], approximate=False).astype(jnp.bfloat16)
                names, block = [0], hidden
                for bit in reversed(order):
                    names = names + [b ^ bit for b in names]
                    more = over_rows(block, bit)
                    block = jnp.concatenate([block, more], axis=0)
                places = {b: n for n, b in enumerate(names)}
                if names != sorted(names):
                    block = jnp.concatenate([block[places[b] * rows_here : (places[b] + 1) * rows_here] for b in range(rows)], axis=0)
                terms = terms + jnp.dot(block, weight_out[cols], preferred_element_type=jnp.float32)

            terms = [terms[:, n * width : (n + 1) * width] for n in range(per_row * CORES)]
            lower, upper = joined(terms[0::CORES], 1), joined(terms[1::CORES], 1)
            taken = over_cores(jnp.where(first, upper, lower).astype(jnp.bfloat16))
            total = jnp.where(first, lower, upper) + taken.astype(jnp.float32)
            backs = []
            for flip in range(rows):
                piece = total[flip * rows_here : (flip + 1) * rows_here].astype(jnp.bfloat16)
                backs.append(over_rows(piece, flip) if flip else piece)
            blocks = jnp.stack(backs).reshape(rows, rows_here, per_row, width)
            blocks = jnp.moveaxis(blocks, 2, 1).reshape(depth, rows_here, width)
            parts = []
            for j in range(depth):
                target = (chip - j) % depth
                index = ((target // per_row) ^ row) * per_row + target % per_row
                parts.append(lax.dynamic_index_in_dim(blocks, index, 0, keepdims=False).astype(jnp.float32))
            results.append((as_float[span] + scatter_depth(parts)).astype(jnp.bfloat16))
        return joined(results, 0)

    return body


def solution(mesh):
    rows, mp = mesh.shape["rows"], mesh.shape["mp"]
    inner = make_body(rows, mp)

    return jax.shard_map(
        inner,
        mesh=mesh,
        in_specs=(P("rows", "mp"), P(), P("mp"), P("rows", "mp"), P("mp", "rows")),
        out_specs=P("rows", "mp"),
        check_vma=False,
    )
```

```python
import jax
import jax.numpy as jnp
from jax import lax
from jax.sharding import PartitionSpec as P


floor_value = 0.1
CORES = 2
TOKEN_CHUNKS = 2
COLUMN_CHUNKS = 4
HALVES = True


def joined(parts, axis):
    return parts[0] if len(parts) == 1 else jnp.concatenate(parts, axis=axis)


def make_body(rows, mp):
    depth = mp // CORES
    per_row = depth // rows
    bits = [1 << n for n in range(rows.bit_length() - 1)]

    def over_rows(value, flip):
        return lax.ppermute(value, "rows", [(i, i ^ flip) for i in range(rows)])

    def over_cores(value):
        return lax.ppermute(value, "mp", [(i, i ^ 1) for i in range(mp)])

    def spread(value, j):
        pairs = []
        for r in range(rows):
            for m in range(mp):
                z, core = divmod(m, CORES)
                target = (r * per_row + z % per_row) ^ j
                pairs.append((r * mp + m, (z // per_row) * mp + target * CORES + core))
        return lax.ppermute(value, ("rows", "mp"), pairs)

    def scatter_depth(parts):
        size = parts[0].shape[0]
        held = dict(enumerate(parts))
        for bit in [1 << n for n in range(depth.bit_length() - 1)]:
            going = [b for b in held if b & bit]
            sent = jnp.concatenate([held[b].astype(jnp.bfloat16) for b in going], axis=0)
            sent = lax.ppermute(sent, "mp", [(i, i ^ (CORES * bit)) for i in range(mp)])
            held = {b ^ bit: held[b ^ bit] + sent[k * size : (k + 1) * size].astype(jnp.float32) for k, b in enumerate(going)}
        return held[0]

    def body(tokens, norm_gain, hidden_bias, weight_in, weight_out):
        count, width = tokens.shape
        hidden_width = weight_in.shape[1]
        features = width * mp
        row, place = lax.axis_index("rows"), lax.axis_index("mp")
        core, chip = place % CORES, place // CORES
        first = core == 0

        as_float = tokens.astype(jnp.float32)
        sums = jnp.stack([jnp.sum(as_float, axis=1), jnp.sum(as_float * as_float, axis=1)])
        sums = lax.all_to_all(jnp.broadcast_to(sums, (rows * mp,) + sums.shape), ("rows", "mp"), 0, 0)
        sums = jnp.sum(sums.reshape((rows, mp) + sums.shape[1:]), axis=1)
        sums = jnp.stack([lax.dynamic_index_in_dim(sums, row ^ flip, 0, keepdims=False) for flip in range(rows)])
        row_mean = sums[:, 0] / features
        row_var = jnp.maximum(sums[:, 1] / features - row_mean * row_mean, 0.0)
        inverse = lax.rsqrt(row_var + floor_value)

        gains = lax.dynamic_slice_in_dim(norm_gain, row * (features // rows), features // rows).reshape(per_row, CORES, width)
        gains = lax.dynamic_index_in_dim(gains, core, 1, keepdims=False)

        got = []
        for j in range(depth):
            got.append(spread(tokens, j))
        stacked = jnp.stack(got)
        pieces = []
        for flip in range(rows):
            parts = []
            for sub in range(per_row):
                at = ((row ^ flip) * per_row + sub) ^ chip
                raw = lax.dynamic_index_in_dim(stacked, at, 0, keepdims=False).astype(jnp.float32)
                scaled = (raw - row_mean[flip][:, None]) * inverse[flip][:, None] * gains[sub][None, :]
                parts.append(scaled.astype(jnp.bfloat16))
            pieces.append(parts)
        x_own = joined([jnp.concatenate([p[sub] for p in pieces], axis=0) for sub in range(per_row)], 1)
        x_other = over_cores(x_own)

        if HALVES:
            blocks_in = weight_in.reshape(per_row, CORES, width, hidden_width)
            w_own = lax.dynamic_index_in_dim(blocks_in, core, 1, keepdims=False).reshape(per_row * width, hidden_width)
            w_other = lax.dynamic_index_in_dim(blocks_in, 1 - core, 1, keepdims=False).reshape(per_row * width, hidden_width)
            w_own, w_other = lax.optimization_barrier((w_own, w_other))
            x_all = [x.reshape(rows, count, per_row * width) for x in (x_own, x_other)]
            w_all = [w_own, w_other]
        else:
            columns = []
            for sub in range(per_row):
                at = slice(sub * width, (sub + 1) * width)
                columns.append(jnp.where(first, x_own[:, at], x_other[:, at]))
                columns.append(jnp.where(first, x_other[:, at], x_own[:, at]))
            x_all = [jnp.concatenate(columns, axis=1).reshape(rows, count, features // rows)]
            w_all = [weight_in]

        cols_here = hidden_width // COLUMN_CHUNKS
        results = []
        for t in range(TOKEN_CHUNKS):
            rows_here = count // TOKEN_CHUNKS
            span = slice(t * rows_here, (t + 1) * rows_here)
            terms = 0.0
            for c in range(COLUMN_CHUNKS):
                cols = slice(c * cols_here, (c + 1) * cols_here)
                turn = (c + t) % len(bits)
                order = bits[turn:] + bits[:turn]
                part = 0.0
                for x, w in zip(x_all, w_all):
                    x = x[:, span].reshape(rows * rows_here, x.shape[2])
                    part = part + jnp.dot(x, w[:, cols], preferred_element_type=jnp.float32)
                held = {b: part[b * rows_here : (b + 1) * rows_here] for b in range(rows)}
                for bit in order:
                    going = [b for b in held if b & bit]
                    sent = over_rows(jnp.concatenate([held[b].astype(jnp.bfloat16) for b in going], axis=0), bit)
                    held = {
                        b ^ bit: held[b ^ bit] + sent[k * rows_here : (k + 1) * rows_here].astype(jnp.float32)
                        for k, b in enumerate(going)
                    }
                hidden = jax.nn.gelu(held[0] + hidden_bias[None, cols], approximate=False).astype(jnp.bfloat16)
                names, block = [0], hidden
                for bit in reversed(order):
                    names = names + [b ^ bit for b in names]
                    more = over_rows(block, bit)
                    block = jnp.concatenate([block, more], axis=0)
                places = {b: n for n, b in enumerate(names)}
                if names != sorted(names):
                    block = jnp.concatenate([block[places[b] * rows_here : (places[b] + 1) * rows_here] for b in range(rows)], axis=0)
                terms = terms + jnp.dot(block, weight_out[cols], preferred_element_type=jnp.float32)

            terms = [terms[:, n * width : (n + 1) * width] for n in range(per_row * CORES)]
            lower, upper = joined(terms[0::CORES], 1), joined(terms[1::CORES], 1)
            taken = over_cores(jnp.where(first, upper, lower).astype(jnp.bfloat16))
            total = jnp.where(first, lower, upper) + taken.astype(jnp.float32)
            backs = []
            for flip in range(rows):
                piece = total[flip * rows_here : (flip + 1) * rows_here].astype(jnp.bfloat16)
                backs.append(over_rows(piece, flip) if flip else piece)
            blocks = jnp.stack(backs).reshape(rows, rows_here, per_row, width)
            blocks = jnp.moveaxis(blocks, 2, 1).reshape(depth, rows_here, width)
            parts = []
            for j in range(depth):
                target = chip ^ j
                index = ((target // per_row) ^ row) * per_row + target % per_row
                parts.append(lax.dynamic_index_in_dim(blocks, index, 0, keepdims=False).astype(jnp.float32))
            results.append((as_float[span] + scatter_depth(parts)).astype(jnp.bfloat16))
        return joined(results, 0)

    return body


def solution(mesh):
    rows, mp = mesh.shape["rows"], mesh.shape["mp"]
    inner = make_body(rows, mp)

    return jax.shard_map(
        inner,
        mesh=mesh,
        in_specs=(P("rows", "mp"), P(), P("mp"), P("rows", "mp"), P("mp", "rows")),
        out_specs=P("rows", "mp"),
        check_vma=False,
    )
```
